8 devices in a mesh: part: 1 (over z), row: 2 (over y), col: 4 (over x, core).
Axes of the slice: x: 2, y: 2, z: 1, core: 2. Of those that a mesh axis runs over, the one named last changes fastest.
Arguments:
- counts: bfloat16 [8192, 16384], P(('part', 'row'), 'col')
- w_init: float32 [8192, 768], P(('part', 'row'))
- h_init: float32 [768, 16384], P(None, ('part', 'col'))
Outputs:
- output 1: float32 [8192, 768], P(('part', 'row'))
- output 2: float32 [768, 16384], P(None, ('part', 'col'))
All inputs are finite; a program needn't handle non-finite values.
Results may differ from the reference program's by a relative error of at most 0.001.
Values are sent between devices in bfloat16 or wider.
A program may use at most 1 GiB of HBM per device.

```python
import jax
import jax.numpy as jnp
from jax import lax

ROW_DEVS = 2
COL_DEVS = 4
DOC_DEV = 4096
WORD_DEV = 4096
TOPICS = 768
SWEEPS = 4
LATENT = 8

DOCS = ROW_DEVS * DOC_DEV
WORDS = COL_DEVS * WORD_DEV
EPS = 1e-6


def setup_inputs(seed: int = 0, part: int = 0) -> dict:
    base_key = jax.random.fold_in(jax.random.key(seed), part)
    sub_keys = jax.random.split(base_key, 7)
    w_true = jax.random.randint(sub_keys[0], (DOCS, LATENT), 0, 4)
    h_true = jax.random.randint(sub_keys[1], (LATENT, WORDS), 0, 4)
    noise_int = jax.random.randint(sub_keys[2], (DOCS, WORDS), -3, 4)
    counts = jnp.clip(jnp.dot(w_true, h_true) + noise_int, 0, 256).astype(jnp.bfloat16)
    init_scale = 4.0 * TOPICS ** -0.5
    w_gain = 2.0 ** jax.random.uniform(sub_keys[3], (1, TOPICS), jnp.float32, -1.0, 1.0)
    h_gain = 2.0 ** jax.random.uniform(sub_keys[4], (TOPICS, 1), jnp.float32, -1.0, 1.0)
    w_init = jax.random.uniform(sub_keys[5], (DOCS, TOPICS), jnp.float32, 0.5, 1.5) * w_gain * init_scale
    h_init = jax.random.uniform(sub_keys[6], (TOPICS, WORDS), jnp.float32, 0.5, 1.5) * h_gain * init_scale
    return {'counts': counts, 'w_init': w_init.astype(jnp.float32), 'h_init': h_init.astype(jnp.float32)}


def ratio_block(c_blk, w_blk, h_blk):
    z_blk = jnp.dot(w_blk, h_blk, preferred_element_type=jnp.float32)
    return (c_blk.astype(jnp.float32) / (z_blk + EPS)).astype(jnp.bfloat16)


def update_w(w_cur, h_cur, c_by_row):
    w_blocks = w_cur.astype(jnp.bfloat16).reshape(ROW_DEVS, DOC_DEV, TOPICS)
    h_blocks = h_cur.astype(jnp.bfloat16).reshape(TOPICS, COL_DEVS, WORD_DEV).transpose(1, 0, 2)

    def one_row(row_items):
        w_blk, c_row = row_items

        def col_step(running, col_items):
            h_blk, c_blk = col_items
            q_blk = ratio_block(c_blk, w_blk, h_blk)
            return running + jnp.dot(q_blk, h_blk.T, preferred_element_type=jnp.float32), None

        total, _ = lax.scan(col_step, jnp.zeros((DOC_DEV, TOPICS), jnp.float32), (h_blocks, c_row))
        return total

    a_w = lax.map(one_row, (w_blocks, c_by_row)).reshape(DOCS, TOPICS)
    s_h = jnp.sum(h_cur, axis=1)
    return w_cur * a_w / s_h[None, :]


def update_h(w_cur, h_cur, c_by_col):
    w_blocks = w_cur.astype(jnp.bfloat16).reshape(ROW_DEVS, DOC_DEV, TOPICS)
    h_blocks = h_cur.astype(jnp.bfloat16).reshape(TOPICS, COL_DEVS, WORD_DEV).transpose(1, 0, 2)

    def one_col(col_items):
        h_blk, c_col = col_items

        def row_step(running, row_items):
            w_blk, c_blk = row_items
            q_blk = ratio_block(c_blk, w_blk, h_blk)
            return running + jnp.dot(w_blk.T, q_blk, preferred_element_type=jnp.float32), None

        total, _ = lax.scan(row_step, jnp.zeros((TOPICS, WORD_DEV), jnp.float32), (w_blocks, c_col))
        return total

    a_h = lax.map(one_col, (h_blocks, c_by_col)).transpose(1, 0, 2).reshape(TOPICS, WORDS)
    s_w = jnp.sum(w_cur, axis=0)
    return h_cur * a_h / s_w[:, None]


def reference(counts, w_init, h_init):
    c_blocks = counts.reshape(ROW_DEVS, DOC_DEV, COL_DEVS, WORD_DEV)
    c_by_row = c_blocks.transpose(0, 2, 1, 3)
    c_by_col = c_blocks.transpose(2, 0, 1, 3)

    def one_sweep(state, unused):
        w_cur, h_cur = state
        w_cur = update_w(w_cur, h_cur, c_by_row)
        h_cur = update_h(w_cur, h_cur, c_by_col)
        return (w_cur, h_cur), None

    (w_out, h_out), _ = lax.scan(one_sweep, (w_init, h_init), None, length=SWEEPS)
    return (w_out, h_out)
```

```python
import functools

import jax
import jax.numpy as jnp
from jax import lax
from jax.experimental import pallas as pl
from jax.experimental.pallas import tpu as pltpu
from jax.sharding import Mesh, PartitionSpec as P

SWEEPS = 4
EPS = 1e-6
CHUNKS = 4
F32 = jnp.float32
BF16 = jnp.bfloat16
MIB = 2 ** 20
ALL = ('y', 'x', 'c')
MESH = pl.DeviceIdType.MESH
CONTRACT_WORDS = (((1,), (1,)), ((), ()))
CONTRACT_DOCS = (((0,), (0,)), ((), ()))


def ratio(c_tile, z_tile):
    return (c_tile.astype(F32) / (z_tile + EPS)).astype(BF16)


def w_kernel(tile, idx_ref, c_ref, w_ref, ho_ref, hs_ref, ka_ref, sa_ref, kb_ref, sb_ref, acc_ref):
    step = pl.program_id(0)
    words = c_ref.shape[1]
    half = w_ref.shape[0] // 2
    for t in range(words // tile):
        cols = pl.ds(t * tile, tile)
        h = jnp.concatenate([ho_ref[:, cols], hs_ref[:, cols]], axis=0)
        z = jnp.dot(w_ref[...], h, preferred_element_type=F32)
        q = ratio(c_ref[:, cols], z)
        part = lax.dot_general(q, h, CONTRACT_WORDS, preferred_element_type=F32)
        if t == 0:
            acc_ref[...] = part
        else:
            acc_ref[...] += part

    @pl.when(step < 2)
    def _():
        sa_ref[0] = acc_ref[:half]

    @pl.when(step >= 2)
    def _():
        ka_ref[0] = acc_ref[:half]

    @pl.when(step % 2 == 0)
    def _():
        sb_ref[0] = acc_ref[half:]

    @pl.when(step % 2 == 1)
    def _():
        kb_ref[0] = acc_ref[half:]


def w_partial(rows, c, w, h_own, h_sib, base):
    words, topics = c.shape[1], w.shape[1]
    idx = jnp.stack([rows[0] + base[0], rows[1] + base[0], rows[2] + base[0], rows[3] + base[0],
                     rows[0] + base[1], rows[1] + base[1], rows[2] + base[1], rows[3] + base[1]])
    part = jax.ShapeDtypeStruct((2, 128, topics), F32)
    block = (1, 128, topics)
    flops = 4 * 1024 * words * topics
    return pl.pallas_call(
        functools.partial(w_kernel, 1024),
        out_shape=(part,) * 4,
        grid_spec=pltpu.PrefetchScalarGridSpec(
            num_scalar_prefetch=1,
            grid=(4,),
            in_specs=[
                pl.BlockSpec((256, words), lambda i, s: (s[i], 0)),
                pl.BlockSpec((256, topics), lambda i, s: (s[4 + i], 0)),
                pl.BlockSpec((topics // 2, words), lambda i, s: (0, 0)),
                pl.BlockSpec((topics // 2, words), lambda i, s: (0, 0)),
            ],
            out_specs=[
                pl.BlockSpec(block, lambda i, s: (i // 3, 0, 0)),
                pl.BlockSpec(block, lambda i, s: (jnp.minimum(i, 1), 0, 0)),
                pl.BlockSpec(block, lambda i, s: (i // 2, 0, 0)),
                pl.BlockSpec(block, lambda i, s: (i // 2, 0, 0)),
            ],
            scratch_shapes=[pltpu.VMEM((256, topics), F32)],
        ),
        cost_estimate=pl.CostEstimate(flops=flops, bytes_accessed=20 * MIB, transcendentals=0),
        compiler_params=pltpu.CompilerParams(dimension_semantics=('arbitrary',), vmem_limit_bytes=56 * MIB),
        name='w_partial',
    )(idx, c, w, h_own, h_sib)


def h_kernel(tile, first, row_ref, c_ref, *refs):
    pieces, refs = refs[:8], refs[8:]
    ho_ref, hs_ref, refs = refs[0], refs[1], refs[2:]
    if not first:
        ik_ref, is_ref, refs = refs[0], refs[1], refs[2:]
    keep_ref, send_ref, w_ref = refs
    own = ho_ref.shape[0]

    @pl.when(pl.program_id(0) == 0)
    def _():
        for quarter in range(4):
            row = pl.multiple_of(row_ref[quarter] * 256, 256)
            w_ref[pl.ds(row, 128), :] = pieces[2 * quarter][...]
            w_ref[pl.ds(row + 128, 128), :] = pieces[2 * quarter + 1][...]

    h = jnp.concatenate([ho_ref[...], hs_ref[...]], axis=0)
    for t in range(c_ref.shape[0] // tile):
        rows = pl.ds(t * tile, tile)
        w = w_ref[rows, :]
        z = jnp.dot(w, h, preferred_element_type=F32)
        q = ratio(c_ref[rows, :], z)
        part = lax.dot_general(w, q, CONTRACT_DOCS, preferred_element_type=F32)
        if t == 0 and first:
            keep_ref[...] = part[:own]
            send_ref[...] = part[own:]
        elif t == 0:
            keep_ref[...] = ik_ref[...] + part[:own]
            send_ref[...] = is_ref[...] + part[own:]
        else:
            keep_ref[...] += part[:own]
            send_ref[...] += part[own:]


def h_partial(rows, c, pieces, h_own, h_sib, sums):
    docs, words = c.shape
    own, topics = h_own.shape[0], 2 * h_own.shape[0]
    width = 1024
    first = sums is None
    spec_h = pl.BlockSpec((own, width), lambda i, s: (0, i))
    in_specs = [pl.BlockSpec((docs, width), lambda i, s: (0, i))]
    in_specs += [pl.BlockSpec((128, topics), lambda i, s: (0, 0))] * 8
    in_specs += [spec_h] * (2 if first else 4)
    acc = jax.ShapeDtypeStruct((own, words), F32)
    return pl.pallas_call(
        functools.partial(h_kernel, 512, first),
        out_shape=(acc, acc, jax.ShapeDtypeStruct((docs, topics), BF16)),
        grid_spec=pltpu.PrefetchScalarGridSpec(
            num_scalar_prefetch=1,
            grid=(words // width,),
            in_specs=in_specs,
            out_specs=[spec_h, spec_h, pl.BlockSpec((docs, topics), lambda i, s: (0, 0))],
        ),
        input_output_aliases={} if first else {12: 0, 13: 1},
        cost_estimate=pl.CostEstimate(flops=4 * docs * words * topics, bytes_accessed=40 * MIB, transcendentals=0),
        compiler_params=pltpu.CompilerParams(dimension_semantics=('arbitrary',), vmem_limit_bytes=56 * MIB),
        name='h_partial',
    )(jnp.stack(rows), c, *pieces, h_own, h_sib, *(() if first else sums))


RS1A, RS1B, RS2A, RS2B, AY, AX, BX, BY, AF, BF = range(10)


def sweep_kernel(tile, c0, c1, c2, c3, wold_ref, ho_ref, hs_ref, wsh_ref, sh_ref,
                 keep_ref, send_ref, shard_ref, wout_ref, wsum_ref,
                 cbuf, wbuf, acc, sa, ka, sb, kb, ra, rb, r2a, r2b, wnew, csem, wsem, osem, ssem, rsem):
    c_refs = (c0, c1, c2, c3)
    j, x = lax.axis_index('y'), lax.axis_index('x')
    own = ho_ref.shape[0]
    words = ho_ref.shape[1]

    barrier = pltpu.get_barrier_semaphore()
    for axis, place in (('x', x), ('y', j)):
        pl.semaphore_signal(barrier, inc=1, device_id={axis: 1 - place}, device_id_type=MESH)
    pl.semaphore_wait(barrier, 2)

    def remote(src, dst, chunk, event, axis):
        other = 1 - (x if axis == 'x' else j)
        return pltpu.make_async_remote_copy(src_ref=src, dst_ref=dst, send_sem=ssem.at[chunk, event],
                                            recv_sem=rsem.at[chunk, event], device_id={axis: other},
                                            device_id_type=MESH)

    def rows_of(chunk, u, v, colour):
        return pl.ds(pl.multiple_of(chunk * 1024 + (2 * u + v) * 256 + colour * 128, 128), 128)

    def copy_of(event, chunk):
        if event == RS1A:
            return remote(sa.at[lax.rem(chunk, 2)], ra.at[chunk], chunk, event, 'x')
        if event == RS1B:
            return remote(sb.at[lax.rem(chunk, 2)], rb.at[chunk], chunk, event, 'y')
        if event == RS2A:
            return remote(ka.at[chunk, 0], r2a.at[chunk], chunk, event, 'y')
        if event == RS2B:
            return remote(kb.at[chunk, 0], r2b.at[chunk], chunk, event, 'x')
        if event in (AY, AX):
            part = wnew.at[rows_of(chunk, x, j, 0)]
            return remote(part, part, chunk, event, 'y' if event == AY else 'x')
        if event in (BX, BY):
            part = wnew.at[rows_of(chunk, x, j, 1)]
            return remote(part, part, chunk, event, 'y' if event == BY else 'x')
        if event == AF:
            part = wnew.at[rows_of(chunk, x, 1 - j, 0)]
            return remote(part, part, chunk, event, 'x')
        part = wnew.at[rows_of(chunk, 1 - x, j, 1)]
        return remote(part, part, chunk, event, 'y')

    def first_sums(chunk):
        copy_of(RS1A, chunk).wait_recv()
        ka[chunk] += ra[chunk]
        copy_of(RS2A, chunk).start()
        copy_of(RS1B, chunk).wait_recv()
        kb[chunk] += rb[chunk]
        copy_of(RS2B, chunk).start()

    def update(chunk):
        copy_of(RS2A, chunk).wait_recv()
        new = wsh_ref[chunk, 0] * (ka[chunk, 1] + r2a[chunk]) / sh_ref[...]
        shard_ref[chunk, 0] = new
        wnew[rows_of(chunk, x, j, 0), :] = new.astype(BF16)
        total = jnp.sum(new, axis=0, keepdims=True)
        copy_of(AY, chunk).start()
        copy_of(AX, chunk).start()
        copy_of(RS2B, chunk).wait_recv()
        new = wsh_ref[chunk, 1] * (kb[chunk, 1] + r2b[chunk]) / sh_ref[...]
        shard_ref[chunk, 1] = new
        wnew[rows_of(chunk, x, j, 1), :] = new.astype(BF16)
        wsum_ref[...] += total + jnp.sum(new, axis=0, keepdims=True)
        copy_of(BX, chunk).start()
        copy_of(BY, chunk).start()

    def forward(chunk):
        copy_of(AY, chunk).wait_recv()
        copy_of(AF, chunk).start()
        copy_of(BX, chunk).wait_recv()
        copy_of(BF, chunk).start()

    def arrived(chunk):
        for event in (AX, BY, AF, BF):
            copy_of(event, chunk).wait_recv()

    def quarter_of(step):
        u = jnp.where(step < 2, 1 - x, x)
        v = jnp.where(step % 2 == 0, 1 - j, j)
        return 2 * u + v

    def fetch_c(chunk, row, slot):
        for n in range(4):
            @pl.when(chunk == n)
            def _():
                pltpu.make_async_copy(c_refs[n].at[pl.ds(row, 256)], cbuf.at[slot], csem.at[slot]).start()

    def wait_c(slot):
        pltpu.make_async_copy(c_refs[0].at[pl.ds(0, 256)], cbuf.at[slot], csem.at[slot]).wait()

    def w_copy(chunk, row, slot):
        return pltpu.make_async_copy(wold_ref.at[pl.ds(chunk * 1024 + row, 256)], wbuf.at[slot], wsem.at[slot])

    def fetch_w_unit(unit, slot):
        chunk = unit // 4
        row = pl.multiple_of(quarter_of(lax.rem(unit, 4)) * 256, 256)
        fetch_c(chunk, row, slot)
        w_copy(chunk, row, slot).start()

    fetch_w_unit(jnp.int32(0), 0)
    for ref in (wsum_ref, keep_ref, send_ref):
        ref[...] = jnp.zeros_like(ref)

    def w_unit(unit, carry):
        chunk, step = unit // 4, lax.rem(unit, 4)
        slot = lax.rem(unit, 2)

        @pl.when(unit < 15)
        def _():
            fetch_w_unit(unit + 1, 1 - slot)

        @pl.when(unit == 15)
        def _():
            fetch_c(jnp.int32(0), 0, 1 - slot)

        wait_c(slot)
        w_copy(chunk, 0, slot).wait()
        for t in range(words // tile):
            cols = pl.ds(t * tile, tile)
            h = jnp.concatenate([ho_ref[:, cols], hs_ref[:, cols]], axis=0)
            z = jnp.dot(wbuf[slot], h, preferred_element_type=F32)
            q = ratio(cbuf[slot, :, cols], z)
            part = lax.dot_general(q, h, CONTRACT_WORDS, preferred_element_type=F32)
            if t == 0:
                acc[...] = part
            else:
                acc[...] += part

        @pl.when((chunk >= 2) & (step == 0))
        def _():
            copy_of(RS1A, chunk - 2).wait_send()
            copy_of(RS1B, chunk - 2).wait_send()

        pos = lax.rem(chunk, 2)

        @pl.when(step < 2)
        def _():
            sa[pos, step] = acc[:128]

        @pl.when(step >= 2)
        def _():
            ka[chunk, step - 2] = acc[:128]

        @pl.when(step % 2 == 0)
        def _():
            sb[pos, step // 2] = acc[128:]

        @pl.when(step % 2 == 1)
        def _():
            kb[chunk, step // 2] = acc[128:]

        @pl.when(step == 1)
        def _():
            copy_of(RS1A, chunk).start()

        @pl.when(step == 2)
        def _():
            copy_of(RS1B, chunk).start()

        @pl.when((step == 3) & (chunk >= 1))
        def _():
            first_sums(chunk - 1)
        return carry

    lax.fori_loop(0, 16, w_unit, 0)
    update(0)
    forward(0)
    first_sums(3)
    update(1)
    forward(1)
    update(2)

    def h_unit(unit, carry):
        chunk, step = unit // 4, lax.rem(unit, 4)
        slot = lax.rem(unit, 2)
        row = pl.multiple_of(step * 256, 256)

        @pl.when(unit < 15)
        def _():
            fetch_c((unit + 1) // 4, pl.multiple_of(lax.rem(unit + 1, 4) * 256, 256), 1 - slot)

        @pl.when(step == 0)
        def _():
            arrived(chunk)
            block = pl.ds(pl.multiple_of(chunk * 1024, 1024), 1024)
            pltpu.make_async_copy(wnew.at[block], wout_ref.at[block], osem.at[chunk]).start()

        wait_c(slot)
        w = wnew[pl.ds(pl.multiple_of(chunk * 1024 + row, 256), 256), :]
        for t in range(words // tile):
            cols = pl.ds(t * tile, tile)
            h = jnp.concatenate([ho_ref[:, cols], hs_ref[:, cols]], axis=0)
            z = jnp.dot(w, h, preferred_element_type=F32)
            q = ratio(cbuf[slot, :, cols], z)
            part = lax.dot_general(w, q, CONTRACT_DOCS, preferred_element_type=F32)

            keep_ref[:, cols] += part[:own]
            send_ref[:, cols] += part[own:]

        @pl.when(unit == 1)
        def _():
            update(3)

        @pl.when(unit == 3)
        def _():
            forward(2)

        @pl.when(unit == 5)
        def _():
            forward(3)
        return carry

    lax.fori_loop(0, 16, h_unit, 0)
    for chunk in range(4):
        block = pl.ds(chunk * 1024, 1024)
        pltpu.make_async_copy(wnew.at[block], wout_ref.at[block], osem.at[chunk]).wait()
        for event in range(10):
            if event > 1 or chunk > 1:
                copy_of(event, chunk).wait_send()


def fused_sweep(c_new, w_old, h_own, h_sib, shards, s_h):
    own, words = h_own.shape
    docs, topics = w_old.shape
    vmem, hbm = pl.BlockSpec(memory_space=pltpu.VMEM), pl.BlockSpec(memory_space=pl.ANY)
    acc = jax.ShapeDtypeStruct((own, words), F32)
    part = pltpu.VMEM((4, 2, 128, topics), F32)
    two = pltpu.VMEM((2, 2, 128, topics), F32)
    last = pltpu.VMEM((4, 128, topics), F32)
    dma = pltpu.SemaphoreType.DMA
    return pl.pallas_call(
        functools.partial(sweep_kernel, 1024),
        out_shape=(acc, acc, jax.ShapeDtypeStruct(shards.shape, F32), jax.ShapeDtypeStruct(w_old.shape, BF16),
                   jax.ShapeDtypeStruct((1, topics), F32)),
        in_specs=[hbm] * 5 + [vmem] * 4,
        out_specs=[vmem, vmem, vmem, hbm, vmem],
        scratch_shapes=[
            pltpu.VMEM((2, 256, words), BF16),
            pltpu.VMEM((2, 256, topics), BF16),
            pltpu.VMEM((256, topics), F32),
            two, part, two, part, part, part, last, last,
            pltpu.VMEM((docs, topics), BF16),
            dma((2,)), dma((2,)), dma((4,)), dma((4, 10)), dma((4, 10)),
        ],
        cost_estimate=pl.CostEstimate(flops=8 * docs * words * topics, bytes_accessed=100 * MIB, transcendentals=0),
        compiler_params=pltpu.CompilerParams(collective_id=0, has_side_effects=True, vmem_limit_bytes=67043328),
        name='fused_sweep',
    )(*c_new, w_old, h_own, h_sib, shards, s_h)


def swap(arr, axis):
    return lax.ppermute(arr, axis, [(0, 1), (1, 0)])


def flip(arr, k, axis):
    half = arr.shape[axis] // 2
    return jnp.where(k == 0, arr, jnp.roll(arr, half, axis=axis))


def first_sum(parts, other):
    keep_a, send_a, keep_b, send_b = parts
    got_a, got_b = swap(send_a, 'x'), swap(send_b, other)
    return (keep_a[0] + got_a[0], keep_b[0] + got_b[0]), (keep_a[1] + got_a[1], keep_b[1] + got_b[1])


def second_sum(mid, other):
    (next_a, next_b), (own_a, own_b) = mid
    return own_a + swap(next_a, other), own_b + swap(next_b, 'x')


def gather_pieces(own_a, own_b):
    a0, b0 = own_a.astype(BF16), own_b.astype(BF16)
    a1, b2 = swap(a0, 'y'), swap(b0, 'x')
    a2, b1 = swap(a0, 'x'), swap(b0, 'y')
    a3, b3 = swap(a1, 'x'), swap(b2, 'y')
    return [a0, b0, a1, b1, a2, b2, a3, b3]


def tie(value, *others):
    return lax.optimization_barrier((value,) + others)


def mesh_sum(vec):
    for axis in ('c', 'x', 'y'):
        vec = vec + swap(vec, axis)
    return vec


def local_sweeps(c_blk, w_loc, h_loc):
    j, x, k = (lax.axis_index(axis) for axis in ALL)
    diag = j == k
    docs, topics = w_loc.shape
    words = h_loc.shape[1]
    half = topics // 2
    chunk = docs // CHUNKS
    dev = lambda jj, xx, kk: jj * 4 + xx * 2 + kk
    trade_pairs = [(dev(a, b, 1 - a), dev(1 - a, b, a)) for a in range(2) for b in range(2)]

    def trade(arr):
        return jnp.where(diag, arr, lax.ppermute(arr, ALL, trade_pairs))

    def steps(u, v):
        return [2 * (1 - u) + 1 - v, 2 * (1 - u) + v, 2 * u + 1 - v, 2 * u + v]

    def w_phase(other, part_of, update):
        tag = jnp.zeros((), jnp.int32)
        parts, mids, shards = [], [], []
        for i in range(CHUNKS):
            if i >= 2:
                tag, parts[i - 2] = tie(tag, parts[i - 2])
                mids.append(first_sum(parts[i - 2], other))
                if i >= 3:
                    shards.append(update(i - 3, second_sum(mids[i - 3], other)))
                    tag, mids[-1], shards[-1] = tie(tag, mids[-1], shards[-1])
                else:
                    tag, mids[-1] = tie(tag, mids[-1])
            parts.append(part_of(i, tag))
        return tag, parts, mids, shards

    def finish(other, i, parts, mids, shards, update):
        if len(mids) < CHUNKS:
            mids.append(first_sum(parts[len(mids)], other))
        if len(shards) < len(mids) and len(shards) < CHUNKS:
            n = len(shards)
            shards.append(update(n, second_sum(mids[n], other)))

    early = [trade(c_blk[i * chunk:(i + 1) * chunk]) for i in range(2)]
    h_bf = h_loc.astype(BF16)
    w_bf = w_loc.astype(BF16)
    s_h = jnp.sum(h_loc, axis=1)
    s_h = s_h + swap(s_h, 'c')
    s_h = s_h + swap(s_h, 'x')

    def part_of(i, tag):
        return w_partial(steps(x, k), c_blk, w_bf, h_bf[:half], h_bf[half:], (4 * i + tag, 4 * i + tag))

    def update(i, sums):
        row = i * chunk + 256 * (2 * x + k)
        w_a = lax.dynamic_slice_in_dim(w_loc, row, 128, 0) * sums[0] / s_h
        w_b = lax.dynamic_slice_in_dim(w_loc, row + 128, 128, 0) * sums[1] / s_h
        both = flip(trade(jnp.stack([w_a, w_b])), k, 2)
        return both[0], both[1]

    tag, parts, mids, shards = w_phase('c', part_of, update)
    while len(shards) < CHUNKS:
        finish('c', 0, parts, mids, shards, update)
    h_rel = flip(jnp.where(diag, h_loc, swap(h_loc, 'c')), k, 0)
    h_own = h_rel[:half]
    h_bf_own, h_bf_sib = h_own.astype(BF16), h_rel[half:].astype(BF16)
    pieces = [gather_pieces(*shard) for shard in shards]
    c_late, pieces[-1][6] = tie(c_blk, pieces[-1][6])
    c_new = early + [trade(c_late[i * chunk:(i + 1) * chunk]) for i in range(2, CHUNKS)]

    for sweep in range(SWEEPS):
        if sweep == 0:
            rows = steps(x, j)[::-1]
            sums, w_full = None, []
            for i in range(CHUNKS):
                keep, send, w_chunk = h_partial(rows, c_new[i], pieces[i], h_bf_own, h_bf_sib, sums)
                sums = keep, send
                w_full.append(w_chunk)
            w_full = jnp.concatenate(w_full)
            w_sum = sum(jnp.sum(w_a + w_b, axis=0) for w_a, w_b in shards)
            shards = jnp.stack([jnp.stack(shard) for shard in shards])
        else:
            h_sum = jnp.sum(h_own, axis=1)
            h_sum = flip(jnp.concatenate([h_sum, jnp.zeros_like(h_sum)]), k, 0)
            s_h = flip(mesh_sum(h_sum), k, 0)
            keep, send, shards, w_full, w_sum = fused_sweep(c_new, w_full, h_bf_own, h_bf_sib, shards, s_h[None])
            w_sum = w_sum[0]
        s_w = flip(mesh_sum(flip(w_sum, k, 0)), k, 0)[:half]
        h_own = h_own * (keep + swap(send, 'c')) / s_w[:, None]
        if sweep < SWEEPS - 1:
            h_bf_own = h_own.astype(BF16)
            h_bf_sib = swap(h_bf_own, 'c')

    own = flip(shards, k, 3)
    into = [(dev(1 - a, b, a), dev(a, b, a)) for a in range(2) for b in range(2)]
    cross = [(dev(a, b, a), dev(a, 1 - b, a)) for a in range(2) for b in range(2)]
    aside = [(dev(a, b, a), dev(a, b, 1 - a)) for a in range(2) for b in range(2)]
    from_y = lax.ppermute(own, ALL, into)
    from_x = lax.ppermute(own, ALL, cross)
    from_xy = lax.ppermute(from_y, ALL, cross)
    near = jnp.where(j == 0, jnp.stack([own, from_y], 1), jnp.stack([from_y, own], 1))
    far = jnp.where(j == 0, jnp.stack([from_x, from_xy], 1), jnp.stack([from_xy, from_x], 1))
    w_half = jnp.where(x == 0, jnp.stack([near, far], 1), jnp.stack([far, near], 1)).reshape(docs, topics)
    w_out = jnp.where(diag, w_half, lax.ppermute(w_half, ALL, aside))

    from_y = swap(h_own, 'y')
    mine = jnp.where(diag, h_own, from_y)
    other = swap(jnp.where(diag, from_y, h_own), 'c')
    h_out = jnp.where(k == 0, jnp.concatenate([mine, other]), jnp.concatenate([other, mine]))
    return w_out, h_out


def solution(mesh):
    fine = Mesh(mesh.devices.reshape(2, 2, 2), ALL)
    spec_c = P('y', ('x', 'c'))
    spec_w = P('y', None)
    spec_h = P(None, ('x', 'c'))
    return jax.shard_map(local_sweeps, mesh=fine, in_specs=(spec_c, spec_w, spec_h), out_specs=(spec_w, spec_h), check_vma=False)
```

```python
import functools

import jax
import jax.numpy as jnp
from jax import lax
from jax.experimental import pallas as pl
from jax.experimental.pallas import tpu as pltpu
from jax.sharding import Mesh, PartitionSpec as P

SWEEPS = 4
EPS = 1e-6
F32 = jnp.float32
BF16 = jnp.bfloat16
MIB = 2 ** 20
ALL = ('y', 'x', 'c')
MESH = pl.DeviceIdType.MESH
CONTRACT_WORDS = (((1,), (1,)), ((), ()))
CONTRACT_DOCS = (((0,), (0,)), ((), ()))


def ratio(c_tile, z_tile):
    return (c_tile.astype(F32) / (z_tile + EPS)).astype(BF16)


RS1A, RS1B, RS2A, RS2B, AY, AX, BX, BY, AF, BF, TR = range(11)
BLOCKS = 16


def sweep_kernel(first, tile, *refs):
    if first:
        c_own, w_ref, h1_ref, wsh_ref, sh_ref = refs[:5]
        keep_ref, send_ref, shard_ref, wout_ref, wsum_ref, c_rcv, h2_ref = refs[5:12]
        refs = refs[12:]
    else:
        c_own, c_rcv, w_ref, h1_ref, h2_ref, wsh_ref, sh_ref = refs[:7]
        keep_ref, send_ref, shard_ref, wout_ref, wsum_ref = refs[7:12]
        refs = refs[12:]
    cbuf, wbuf, hbuf, acc, sa, ka, sb, kb, ra, rb, r2a, r2b, wnew, csem, wsem, hsem, osem, ssem, rsem = refs[:19]
    if first:
        tr, cssem, crsem, hrsem = refs[19:]
    j, x, k = (lax.axis_index(axis) for axis in ALL)
    place = {'y': j, 'x': x, 'c': k}
    diag = j == k
    own, words = keep_ref.shape
    second = 'c' if first else 'y'
    v_pos = place[second]

    def flipped(axes):
        return {axis: 1 - place[axis] for axis in axes}

    barrier = pltpu.get_barrier_semaphore()
    greet = (('x',), ('y',), ('c',), ('y', 'c')) if first else (('x',), ('y',))
    for axes in greet:
        pl.semaphore_signal(barrier, inc=1, device_id=flipped(axes), device_id_type=MESH)
    pl.semaphore_wait(barrier, len(greet))

    def remote(src, dst, send, recv, axes):
        return pltpu.make_async_remote_copy(src_ref=src, dst_ref=dst, send_sem=send, recv_sem=recv,
                                            device_id=flipped(axes), device_id_type=MESH)

    def rows_of(chunk, u, v, colour):
        return pl.ds(pl.multiple_of(chunk * 1024 + (2 * u + v) * 256 + colour * 128, 128), 128)

    def copy_of(event, chunk):
        sems = ssem.at[chunk, event], rsem.at[chunk, event]
        pos = lax.rem(chunk, 2)
        if event == RS1A:
            return remote(sa.at[pos], ra.at[chunk], *sems, 'x')
        if event == RS1B:
            return remote(sb.at[pos], rb.at[chunk], *sems, second)
        if event == RS2A:
            return remote(ka.at[chunk, 0], r2a.at[chunk], *sems, second)
        if event == RS2B:
            return remote(kb.at[chunk, 0], r2b.at[chunk], *sems, 'x')
        if event == TR:
            return remote(ra.at[chunk], tr.at[chunk], *sems, 'yc')
        rows = {AY: (x, j, 0), AX: (x, j, 0), BX: (x, j, 1), BY: (x, j, 1), AF: (x, 1 - j, 0), BF: (1 - x, j, 1)}
        part = wnew.at[rows_of(chunk, *rows[event])]
        return remote(part, part, *sems, 'y' if event in (AY, BY, BF) else 'x')

    def first_sums(chunk):
        copy_of(RS1A, chunk).wait_recv()
        ka[chunk] += ra[chunk]
        copy_of(RS2A, chunk).start()
        copy_of(RS1B, chunk).wait_recv()
        kb[chunk] += rb[chunk]
        copy_of(RS2B, chunk).start()

    def publish_a(chunk, new):
        shard_ref[chunk, 0] = new
        wnew[rows_of(chunk, x, j, 0), :] = new.astype(BF16)
        copy_of(AY, chunk).start()
        copy_of(AX, chunk).start()
        wsum_ref[...] += jnp.sum(new, axis=0, keepdims=True)

    def publish_b(chunk, new):
        shard_ref[chunk, 1] = new
        wnew[rows_of(chunk, x, j, 1), :] = new.astype(BF16)
        copy_of(BX, chunk).start()
        copy_of(BY, chunk).start()
        wsum_ref[...] += jnp.sum(new, axis=0, keepdims=True)

    def update(chunk):
        copy_of(RS2A, chunk).wait_recv()
        new = wsh_ref[chunk, 0] * (ka[chunk, 1] + r2a[chunk]) / sh_ref[...]
        if first:
            ra[chunk, 0] = new
        else:
            publish_a(chunk, new)
        copy_of(RS2B, chunk).wait_recv()
        new = wsh_ref[chunk, 1] * (kb[chunk, 1] + r2b[chunk]) / sh_ref[...]
        if first:
            ra[chunk, 1] = new

            @pl.when(jnp.logical_not(diag))
            def _():
                copy_of(TR, chunk).start()
        else:
            publish_b(chunk, new)

    def settle(chunk):
        def turned(ref, colour):
            value = ref[chunk, colour]
            return jnp.where(k == 0, value, jnp.concatenate([value[:, own:], value[:, :own]], axis=1))

        @pl.when(diag)
        def _():
            publish_a(chunk, turned(ra, 0))
            publish_b(chunk, turned(ra, 1))

        @pl.when(jnp.logical_not(diag))
        def _():
            copy_of(TR, chunk).wait_recv()
            publish_a(chunk, turned(tr, 0))
            publish_b(chunk, turned(tr, 1))

    def forward(chunk):
        copy_of(AY, chunk).wait_recv()
        copy_of(AF, chunk).start()
        copy_of(BX, chunk).wait_recv()
        copy_of(BF, chunk).start()

    def arrived(chunk):
        for event in (AX, BY, AF, BF):
            copy_of(event, chunk).wait_recv()

    def trade_of(block):
        rows = pl.ds(pl.multiple_of(block * 256, 256), 256)
        return remote(c_own.at[rows], c_rcv.at[rows], cssem.at[block], crsem.at[block], 'yc')

    def trade_start(block):
        @pl.when(jnp.logical_not(diag))
        def _():
            trade_of(block).start()

    def h_trade():
        return remote(h1_ref, h2_ref, hrsem.at[0], hrsem.at[1], 'c')

    def quarter_of(step):
        u = jnp.where(step < 2, 1 - x, x)
        v = jnp.where(step % 2 == 0, 1 - v_pos, v_pos)
        return 2 * u + v

    def c_copy(ref, row, slot):
        return pltpu.make_async_copy(ref.at[pl.ds(row, 256)], cbuf.at[slot], csem.at[slot])

    def fetch_c(row, slot, products):
        if first and products:
            c_copy(c_own, row, slot).start()
            return

        @pl.when(diag)
        def _():
            c_copy(c_own, row, slot).start()

        @pl.when(jnp.logical_not(diag))
        def _():
            if first:
                trade_of(row // 256).wait_recv()
            c_copy(c_rcv, row, slot).start()

    def w_copy(row, slot):
        return pltpu.make_async_copy(w_ref.at[pl.ds(row, 256)], wbuf.at[slot], wsem.at[slot])

    def fetch_w_unit(unit, slot):
        row = pl.multiple_of((unit // 4) * 1024 + quarter_of(lax.rem(unit, 4)) * 256, 256)
        fetch_c(row, slot, True)
        w_copy(row, slot).start()

    def h_copies(own_ref, sib_ref, own_row, sib_row):
        return [pltpu.make_async_copy(ref.at[pl.ds(pl.multiple_of(row, own), own)], hbuf.at[pl.ds(n * own, own)],
                                      hsem.at[n])
                for n, (ref, row) in enumerate(((own_ref, own_row), (sib_ref, sib_row)))]

    if first:
        trade_start(0)
        trade_start(1)

        @pl.when(diag)
        def _():
            h_trade().start()
        loads = h_copies(h1_ref, h1_ref, 0, own)
    else:
        loads = h_copies(h1_ref, h2_ref, 0, 0)
    for load in loads:
        load.start()
    fetch_w_unit(jnp.int32(0), 0)
    for ref in (wsum_ref, keep_ref, send_ref):
        ref[...] = jnp.zeros_like(ref)
    for load in loads:
        load.wait()

    def w_unit(unit, carry):
        chunk, step = unit // 4, lax.rem(unit, 4)
        slot = lax.rem(unit, 2)

        @pl.when(unit < BLOCKS - 1)
        def _():
            fetch_w_unit(unit + 1, 1 - slot)

        c_copy(c_own, 0, slot).wait()
        w_copy(0, slot).wait()
        for t in range(words // tile):
            cols = pl.ds(t * tile, tile)
            h = hbuf[:, cols]
            z = jnp.dot(wbuf[slot], h, preferred_element_type=F32)
            q = ratio(cbuf[slot, :, cols], z)
            part = lax.dot_general(q, h, CONTRACT_WORDS, preferred_element_type=F32)
            if t == 0:
                acc[...] = part
            else:
                acc[...] += part

        @pl.when((chunk >= 2) & (step == 0))
        def _():
            copy_of(RS1A, chunk - 2).wait_send()
            copy_of(RS1B, chunk - 2).wait_send()

        pos = lax.rem(chunk, 2)

        @pl.when(step < 2)
        def _():
            sa[pos, step] = acc[:128]

        @pl.when(step >= 2)
        def _():
            ka[chunk, step - 2] = acc[:128]

        @pl.when(step % 2 == 0)
        def _():
            sb[pos, step // 2] = acc[128:]

        @pl.when(step % 2 == 1)
        def _():
            kb[chunk, step // 2] = acc[128:]

        @pl.when(step == 1)
        def _():
            copy_of(RS1A, chunk).start()

        @pl.when(step == 2)
        def _():
            copy_of(RS1B, chunk).start()

        if first:
            @pl.when(lax.rem(unit, 3) == 2)
            def _():
                trade_start(2 + unit // 3)

        @pl.when((step == 3) & (chunk >= 1))
        def _():
            first_sums(chunk - 1)
        return carry

    lax.fori_loop(0, BLOCKS, w_unit, 0)
    if first:
        def next_loads(ref):
            return h_copies(ref, ref, k * own, (1 - k) * own)

        @pl.when(diag)
        def _():
            for load in next_loads(h1_ref):
                load.start()

        @pl.when(jnp.logical_not(diag))
        def _():
            h_trade().wait_recv()
            for load in next_loads(h2_ref):
                load.start()

        update(0)
        trade_start(7)
        first_sums(3)
        for chunk in range(1, 4):
            update(chunk)
            trade_start(7 + chunk)
        for chunk in range(4):
            settle(chunk)
            trade_start(11 + chunk)
        for chunk in range(4):
            forward(chunk)
            if chunk == 0:
                trade_start(15)
        for load in next_loads(h1_ref):
            load.wait()
    else:
        update(0)
        forward(0)
        first_sums(3)
        update(1)
        forward(1)
        update(2)
    fetch_c(0, 0, False)

    def h_unit(unit, carry):
        chunk = unit // 4
        slot = lax.rem(unit, 2)

        @pl.when(unit < BLOCKS - 1)
        def _():
            fetch_c(pl.multiple_of((unit + 1) * 256, 256), 1 - slot, False)

        @pl.when(lax.rem(unit, 4) == 0)
        def _():
            arrived(chunk)
            block = pl.ds(pl.multiple_of(chunk * 1024, 1024), 1024)
            pltpu.make_async_copy(wnew.at[block], wout_ref.at[block], osem.at[chunk]).start()

        c_copy(c_own, 0, slot).wait()
        w = wnew[pl.ds(pl.multiple_of(unit * 256, 256), 256), :]
        for t in range(words // tile):
            cols = pl.ds(t * tile, tile)
            z = jnp.dot(w, hbuf[:, cols], preferred_element_type=F32)
            q = ratio(cbuf[slot, :, cols], z)
            part = lax.dot_general(w, q, CONTRACT_DOCS, preferred_element_type=F32)
            keep_ref[:, cols] += part[:own]
            send_ref[:, cols] += part[own:]

        if not first:
            @pl.when(unit == 1)
            def _():
                update(3)

            @pl.when(unit == 3)
            def _():
                forward(2)

            @pl.when(unit == 5)
            def _():
                forward(3)
        return carry

    lax.fori_loop(0, BLOCKS, h_unit, 0)
    for chunk in range(4):
        block = pl.ds(chunk * 1024, 1024)
        pltpu.make_async_copy(wnew.at[block], wout_ref.at[block], osem.at[chunk]).wait()
        for event in range(10):
            if event > 1 or chunk > 1:
                copy_of(event, chunk).wait_send()
    if first:
        @pl.when(diag)
        def _():
            h_trade().wait_send()

        @pl.when(jnp.logical_not(diag))
        def _():
            for chunk in range(4):
                copy_of(TR, chunk).wait_send()
            for block in range(BLOCKS):
                trade_of(block).wait_send()


def fused_sweep(first, arrays, shards, s_h):
    docs, words, topics = 4096, 4096, shards.shape[-1]
    vmem, hbm = pl.BlockSpec(memory_space=pltpu.VMEM), pl.BlockSpec(memory_space=pl.ANY)
    acc = jax.ShapeDtypeStruct((topics // 2, words), F32)
    part = pltpu.VMEM((4, 2, 128, topics), F32)
    two = pltpu.VMEM((2, 2, 128, topics), F32)
    last = pltpu.VMEM((4, 128, topics), F32)
    dma = pltpu.SemaphoreType.DMA
    outs = (acc, acc, jax.ShapeDtypeStruct(shards.shape, F32), jax.ShapeDtypeStruct((docs, topics), BF16),
            jax.ShapeDtypeStruct((1, topics), F32))
    scratch = [
        pltpu.VMEM((2, 256, words), BF16),
        pltpu.VMEM((2, 256, topics), BF16),
        pltpu.VMEM((topics, words), BF16),
        pltpu.VMEM((256, topics), F32),
        two, part, two, part, part, part, last, last,
        pltpu.VMEM((docs, topics), BF16),
        dma((2,)), dma((2,)), dma((2,)), dma((4,)), dma((4, 11)), dma((4, 11)),
    ]
    out_specs = [vmem, vmem, vmem, hbm, vmem]
    if first:
        outs += (jax.ShapeDtypeStruct((docs, words), BF16), jax.ShapeDtypeStruct((topics, words), BF16))
        out_specs += [hbm, hbm]
        scratch += [part, dma((BLOCKS,)), dma((BLOCKS,)), dma((2,))]
    return pl.pallas_call(
        functools.partial(sweep_kernel, first, 1024),
        out_shape=outs,
        in_specs=[hbm] * len(arrays) + [vmem] * 2,
        out_specs=out_specs,
        scratch_shapes=scratch,
        cost_estimate=pl.CostEstimate(flops=8 * docs * words * topics, bytes_accessed=100 * MIB, transcendentals=0),
        compiler_params=pltpu.CompilerParams(collective_id=int(first), has_side_effects=True,
                                             vmem_limit_bytes=67043328),
        name='first_sweep' if first else 'fused_sweep',
    )(*arrays, shards, s_h)


def swap(arr, axis):
    return lax.ppermute(arr, axis, [(0, 1), (1, 0)])


def flip(arr, k, axis):
    half = arr.shape[axis] // 2
    return jnp.where(k == 0, arr, jnp.roll(arr, half, axis=axis))


def mesh_sum(vec):
    for axis in ('c', 'x', 'y'):
        vec = vec + swap(vec, axis)
    return vec


def local_sweeps(c_blk, w_loc, h_loc):
    j, x, k = (lax.axis_index(axis) for axis in ALL)
    diag = j == k
    docs, topics = w_loc.shape
    half = topics // 2
    dev = lambda jj, xx, kk: jj * 4 + xx * 2 + kk

    s_h = jnp.sum(h_loc, axis=1)
    s_h = s_h + swap(s_h, 'c')
    s_h = s_h + swap(s_h, 'x')
    h_bf = h_loc.astype(BF16)
    w_bf = w_loc.astype(BF16)
    shards = lax.dynamic_slice_in_dim(w_loc.reshape(4, 4, 2, 128, topics), 2 * x + k, 1, 1)[:, 0]
    wanted = lax.dynamic_slice_in_dim(h_loc, (1 - k) * half, half, 0)
    h_own = jnp.where(diag, lax.dynamic_slice_in_dim(h_loc, k * half, half, 0), swap(wanted, 'c'))

    for sweep in range(SWEEPS):
        if sweep == 0:
            keep, send, shards, w_bf, w_sum, c_rcv, unused = fused_sweep(True, (c_blk, w_bf, h_bf), shards, s_h[None])
        else:
            h_sum = jnp.sum(h_own, axis=1)
            h_sum = flip(jnp.concatenate([h_sum, jnp.zeros_like(h_sum)]), k, 0)
            s_h = flip(mesh_sum(h_sum), k, 0)
            keep, send, shards, w_bf, w_sum = fused_sweep(
                False, (c_blk, c_rcv, w_bf, h_bf_own, h_bf_sib), shards, s_h[None])
        s_w = flip(mesh_sum(flip(w_sum[0], k, 0)), k, 0)[:half]
        h_own = h_own * (keep + swap(send, 'c')) / s_w[:, None]
        if sweep < SWEEPS - 1:
            h_bf_own = h_own.astype(BF16)
            h_bf_sib = swap(h_bf_own, 'c')

    own = flip(shards, k, 3)
    into = [(dev(1 - a, b, a), dev(a, b, a)) for a in range(2) for b in range(2)]
    cross = [(dev(a, b, a), dev(a, 1 - b, a)) for a in range(2) for b in range(2)]
    aside = [(dev(a, b, a), dev(a, b, 1 - a)) for a in range(2) for b in range(2)]
    from_y = lax.ppermute(own, ALL, into)
    from_x = lax.ppermute(own, ALL, cross)
    from_xy = lax.ppermute(from_y, ALL, cross)
    near = jnp.where(j == 0, jnp.stack([own, from_y], 1), jnp.stack([from_y, own], 1))
    far = jnp.where(j == 0, jnp.stack([from_x, from_xy], 1), jnp.stack([from_xy, from_x], 1))
    w_half = jnp.where(x == 0, jnp.stack([near, far], 1), jnp.stack([far, near], 1)).reshape(docs, topics)
    w_out = jnp.where(diag, w_half, lax.ppermute(w_half, ALL, aside))

    from_y = swap(h_own, 'y')
    mine = jnp.where(diag, h_own, from_y)
    other = swap(jnp.where(diag, from_y, h_own), 'c')
    h_out = jnp.where(k == 0, jnp.concatenate([mine, other]), jnp.concatenate([other, mine]))
    return w_out, h_out


def solution(mesh):
    fine = Mesh(mesh.devices.reshape(2, 2, 2), ALL)
    spec_c = P('y', ('x', 'c'))
    spec_w = P('y', None)
    spec_h = P(None, ('x', 'c'))
    return jax.shard_map(local_sweeps, mesh=fine, in_specs=(spec_c, spec_w, spec_h), out_specs=(spec_w, spec_h), check_vma=False)
```
